32 devices in a mesh: row: 4 (over z), col: 8 (over y, x, core).
Axes of the slice: x: 2, y: 2, z: 4, core: 2. Of those that a mesh axis runs over, the one named last changes fastest.
Arguments:
- grad_terms: bfloat16 [8, 2, 4096, 10240], P('col', None, 'row'), may hold values from -25 to 25, as said below
- row_moment: float32 [2, 4096], P(None, 'row'), may hold values from 0.01 to 3
- col_moment: float32 [2, 10240], P(None, 'col'), may hold values from 0.01 to 1
Outputs:
- update: float32 [2, 4096, 10240], P(None, 'row', 'col')
- new_rows: float32 [2, 4096], P(None, 'row')
- new_cols: float32 [2, 10240], P(None, 'col')
The draws below stay inside these ranges and needn't reach their ends.
Inputs may be any that keep to these rules, and one draw needn't show every extreme that they name: `grad_terms`: partial gradient terms of the 8 batch shards.
All inputs are finite; a program needn't handle non-finite values.
Results may differ from the reference program's by a relative error of at most 0.0003.
Values sent between devices are 32-bit elements; how exact they have to be, the bound alone decides.
No kernel may reach another device: no remote copies, remote signals or barrier semaphores. Data moves between devices by JAX's collectives and lax.ppermute only.
A program may use at most 256 MiB of HBM per device.

```python
import math
import jax
import jax.numpy as jnp
from jax import lax

D = 4096
FF = 10240
MATS = 2
SOURCES = 8


def draw_grad_terms(key, part):
    subkeys = jax.random.split(key, 4)
    full_shape = (SOURCES, MATS, D, FF)
    chosen = jax.random.randint(subkeys[0], (), 0, MATS)
    factor = jnp.where(jnp.arange(MATS) == chosen, 1.0, 0.05).astype(jnp.float32)
    row_scale = jnp.exp(jax.random.uniform(subkeys[1], (MATS, D, 1), jnp.float32, jnp.log(0.3), jnp.log(3.0)))
    col_scale = jnp.exp(jax.random.uniform(subkeys[2], (MATS, 1, FF), jnp.float32, jnp.log(0.3), jnp.log(3.0)))
    base_values = 0.25 * jax.random.truncated_normal(subkeys[3], -4.0, 4.0, full_shape, jnp.float32)
    values = base_values * row_scale[None] * col_scale[None] * factor[None, :, None, None]
    return values.astype(jnp.bfloat16)


def draw_row_moment(key, part):
    subkeys = jax.random.split(jax.random.fold_in(key, 17), 1)
    position = jnp.arange(D, dtype=jnp.float32)[None, :] / jnp.float32(D - 1)
    rough = jnp.exp(jax.random.uniform(subkeys[0], (MATS, D), jnp.float32, jnp.log(0.02), jnp.log(0.2)))
    rising = jnp.exp(position * jnp.log(10.0))
    return (rough * rising).astype(jnp.float32)


def levels(rng, extent, pieces, smallest, top_value):
    def one(dim, shards_of):
        draws = jax.random.uniform(jax.random.fold_in(jax.random.fold_in(rng, 6), dim), (shards_of,), jnp.float32, smallest / len(pieces), top_value / len(pieces))
        return jnp.repeat(jnp.exp(draws), extent[dim] // shards_of).reshape((-1,) + (1,) * (len(extent) - dim - 1))

    gain = one(*pieces[0])
    for cut in pieces[1:]:
        gain = gain * one(*cut)
    return gain


def setup_inputs(seed: int = 0) -> dict:
    keys = jax.random.split(jax.random.key(seed), 4)
    grad_terms = draw_grad_terms(jax.random.fold_in(keys[3], 71), 0)
    row_moment = draw_row_moment(jax.random.fold_in(keys[3], 71), 0)
    col_moment = jnp.clip(jnp.exp(math.log(1.0) - 4.6051702 * jax.random.uniform(keys[2], (MATS, FF), jnp.float32) ** levels(keys[2], (MATS, FF), ((1, 8),), -0.2, 0.2)), 0.01, 1.0)
    return dict(grad_terms=grad_terms, row_moment=row_moment, col_moment=col_moment)


second_decay = 1.0 - 100.0 ** (-0.8)
tiny_square = 1e-30

def reference(grad_terms, row_moment, col_moment):

    def accumulate(source, running):
        return running + grad_terms[source].astype(jnp.float32)
    gradient = lax.fori_loop(0, grad_terms.shape[0], accumulate, jnp.zeros(grad_terms.shape[1:], jnp.float32))
    squares = gradient * gradient + tiny_square
    new_rows = second_decay * row_moment + (1.0 - second_decay) * lax.optimization_barrier(jnp.sum(squares, axis=2)) / FF
    new_cols = second_decay * col_moment + (1.0 - second_decay) * lax.optimization_barrier(jnp.sum(squares, axis=1)) / D
    row_level = lax.optimization_barrier(jnp.sum(new_rows, axis=1)) / D
    estimate = new_rows[:, :, None] * new_cols[:, None, :] / row_level[:, None, None]
    raw_update = gradient / jnp.sqrt(estimate)
    clip_scale = jnp.maximum(1.0, jnp.sqrt(lax.optimization_barrier(jnp.sum(raw_update * raw_update, axis=(1, 2))) / (D * FF)))
    update = raw_update / clip_scale[:, None, None]
    return (update, new_rows, new_cols)
```

```python
import functools

import jax
import jax.numpy as jnp
from jax import lax
from jax.experimental import pallas as pl
from jax.experimental.pallas import tpu as pltpu
from jax.sharding import PartitionSpec as P

second_decay = 1.0 - 100.0 ** (-0.8)
tiny_square = 1e-30


FIRST = (1, 1, 2, 4, 4, 4)
LAST = (4, 4, 4, 2, 2)

ANY = pl.BlockSpec(memory_space=pl.ANY)


def exchange(value, axis, size, mask):
    return lax.ppermute(value, axis, [(i, i ^ mask) for i in range(size)])


def sum_over(value, axis, size):
    mask = 1
    while mask < size:
        value = value + exchange(value, axis, size, mask)
        mask *= 2
    return value


def rows_per_block(rows, most):
    while rows > most:
        rows //= 2
    return rows


def peer_half(table, terms, token, chunk, places, width):
    matrix, start, rows = chunk
    block = rows_per_block(rows, 64)

    def body(table_ref, first, second, token_ref, out):
        out[0] = first[...].astype(jnp.float32)
        out[1] = second[...].astype(jnp.float32)

    def terms_spec(half):
        return pl.BlockSpec(
            (None, None, block, width),
            lambda p, i, t: (matrix, half, start // block + i, t[half, p] ^ 1),
        )

    return pl.pallas_call(
        body,
        grid_spec=pltpu.PrefetchScalarGridSpec(
            num_scalar_prefetch=1,
            grid=(places, rows // block),
            in_specs=[terms_spec(0), terms_spec(1), ANY],
            out_specs=pl.BlockSpec((2, None, block, width), lambda p, i, t: (0, p, i, 0)),
        ),
        out_shape=jax.ShapeDtypeStruct((2, places, rows, width), jnp.float32),
        name="peer_half",
    )(table, terms, terms, token)


def partial_sums(table, terms, from_peer, received, token, chunk, base, width):
    matrix, start, rows = chunk
    block = rows_per_block(rows, 64)
    count = len(received)

    def body(table_ref, *refs):
        first, second, peer = refs[:3]
        others = refs[3 : 3 + 2 * count]
        outs = refs[-2:]
        for half, own in enumerate((first, second)):
            total = own[...].astype(jnp.float32) + peer[half]
            for k in range(count):
                total = total + others[2 * k + half][...]
            outs[half][...] = total

    def terms_spec(half):
        return pl.BlockSpec(
            (None, None, block, width),
            lambda p, i, t: (matrix, half, start // block + i, t[half, base + p]),
        )

    shifted = pl.BlockSpec((None, block, width), lambda p, i, t: (base + p, i, 0))
    plain = pl.BlockSpec((None, block, width), lambda p, i, t: (p, i, 0))
    shape = jax.ShapeDtypeStruct((base, rows, width), jnp.float32)
    return pl.pallas_call(
        body,
        grid_spec=pltpu.PrefetchScalarGridSpec(
            num_scalar_prefetch=1,
            grid=(base, rows // block),
            in_specs=[
                terms_spec(0),
                terms_spec(1),
                pl.BlockSpec((2, None, block, width), lambda p, i, t: (0, base + p, i, 0)),
                *[shifted] * (2 * count),
                ANY,
            ],
            out_specs=[plain, plain],
        ),
        out_shape=[shape, shape],
        name="partial_sums",
    )(table, terms, terms, from_peer, *[r for pair in received for r in pair], token)


def final_sums(table, terms, from_peer, received, gradient, columns, token, chunk, half_rows, width):
    matrix, start, rows = chunk
    count = len(received)
    begin = gradient is None

    def body(table_ref, own, peer, *refs):
        others = refs[: 2 * count]
        rest = refs[2 * count :]
        running = None if begin else rest[1]
        out, row_out, col_out = rest[-3:]
        col_total = jnp.zeros((1, width), jnp.float32) if begin else running[...]
        for half in range(2):
            total = own[half].astype(jnp.float32) + peer[half]
            for k in range(count):
                total = total + others[2 * k + half][...]
            out[half] = total
            squares = total * total + tiny_square
            col_total = col_total + jnp.sum(squares, axis=0, keepdims=True)
            lanes = squares[:, :128]
            for c in range(128, width, 128):
                lanes = lanes + squares[:, c : c + 128]
            row_out[half : half + 1, :] = jnp.sum(lanes.T, axis=0, keepdims=True)
        col_out[...] = col_total

    one = pl.BlockSpec((None, rows, width), lambda i, t: (0, 0, 0))
    whole_row = pl.BlockSpec((1, width), lambda i, t: (0, 0))
    extra = [] if begin else [ANY, whole_row]
    given = [] if begin else [gradient, columns]
    return pl.pallas_call(
        body,
        grid_spec=pltpu.PrefetchScalarGridSpec(
            num_scalar_prefetch=1,
            grid=(1,),
            in_specs=[
                pl.BlockSpec(
                    (None, 2, rows, width), lambda i, t: (matrix, 0, start // rows, t[0, 0])
                ),
                pl.BlockSpec((2, None, rows, width), lambda i, t: (0, 0, 0, 0)),
                *[one] * (2 * count),
                *extra,
                ANY,
            ],
            out_specs=[
                pl.BlockSpec((2, rows, width), lambda i, t: (0, start // rows, 0)),
                pl.BlockSpec((2, rows), lambda i, t: (0, 0)),
                whole_row,
            ],
        ),
        out_shape=[
            jax.ShapeDtypeStruct((2, half_rows, width), jnp.float32),
            jax.ShapeDtypeStruct((2, rows), jnp.float32),
            jax.ShapeDtypeStruct((1, width), jnp.float32),
        ],
        input_output_aliases={} if begin else {3 + 2 * count: 0},
        name="final_sums",
    )(table, terms, from_peer, *[r for pair in received for r in pair], *given, token)


def down_rows(row):
    return jnp.broadcast_to(row, (128, 128)).T


def clip_lanes(gradient, row_factor, col_factor, token, width):
    rows = gradient.shape[0]

    def body(g, r, c, token_ref, out):
        i = pl.program_id(0)

        @pl.when(i == 0)
        def _():
            out[...] = jnp.zeros_like(out)

        factor = down_rows(r[pl.ds(i, 1), :])
        total = jnp.zeros((128, 128), jnp.float32)
        for k in range(0, width, 128):
            scaled = g[:, k : k + 128] * factor * c[:, k : k + 128]
            total = total + scaled * scaled
        out[...] += jnp.sum(total, axis=0, keepdims=True)

    return pl.pallas_call(
        body,
        grid=(rows // 128,),
        in_specs=[
            pl.BlockSpec((128, width), lambda i: (i, 0)),
            pl.BlockSpec((rows // 128, 128), lambda i: (0, 0)),
            pl.BlockSpec((1, width), lambda i: (0, 0)),
            ANY,
        ],
        out_specs=pl.BlockSpec((1, 128), lambda i: (0, 0)),
        out_shape=jax.ShapeDtypeStruct((1, 128), jnp.float32),
        name="clip_lanes",
    )(gradient, row_factor, col_factor, token)


def scale(gradient, row_factor, col_factor, output, token, matrix, mats, width):
    rows = gradient.shape[0]
    begin = output is None

    def body(g, r, c, *refs):
        out = refs[-1]
        factor = down_rows(r[pl.ds(pl.program_id(0), 1), :])
        for k in range(0, width, 128):
            out[:, k : k + 128] = g[:, k : k + 128] * factor * c[:, k : k + 128]

    return pl.pallas_call(
        body,
        grid=(rows // 128,),
        in_specs=[
            pl.BlockSpec((128, width), lambda i: (i, 0)),
            pl.BlockSpec((rows // 128, 128), lambda i: (0, 0)),
            pl.BlockSpec((1, width), lambda i: (0, 0)),
            *([] if begin else [ANY]),
            ANY,
        ],
        out_specs=pl.BlockSpec((None, 128, width), lambda i: (matrix, i, 0)),
        out_shape=jax.ShapeDtypeStruct((mats, rows, width), jnp.float32),
        input_output_aliases={} if begin else {3: 0},
        name="scale",
    )(gradient, row_factor, col_factor, *([] if begin else [output]), token)


def on_device(n_row, n_col, grad_terms, row_moment, col_moment):
    _, mats, rows, all_width = grad_terms.shape
    width = all_width // n_col
    half_rows = rows // 2
    bits = n_col.bit_length() - 2
    places = 1 << bits
    total_rows, total_cols = rows * n_row, all_width

    me = lax.axis_index("col").astype(jnp.int32)
    terms = grad_terms.reshape(mats, 2, half_rows, all_width)
    orders = (tuple(range(bits)), tuple(reversed(range(bits))))

    def place_mask(order, place):
        return sum(1 << bit for k, bit in enumerate(order) if place >> (bits - 1 - k) & 1)

    masks = [[2 * place_mask(order, p) for p in range(places)] for order in orders]
    table = jnp.bitwise_xor(jnp.array(masks, jnp.int32), me)

    chunks = []
    unit = half_rows // 16
    for matrix in range(mats):
        start = 0
        for size in FIRST if matrix == 0 else LAST:
            chunks.append((matrix, start, size * unit))
            start += size * unit
    last_of = {c[0]: i for i, c in enumerate(chunks)}

    from_peer, received = {}, {i: [] for i in range(len(chunks))}
    gradient, columns, row_sums = [None] * mats, [None] * mats, [[] for _ in range(mats)]
    output = None
    new_rows, new_cols = [None] * mats, [None] * mats
    token = table
    pending = []

    def statistics(matrix):
        row_full = sum_over(jnp.concatenate(row_sums[matrix], axis=1), "col", n_col)
        row_full = row_full.reshape(rows // 128, 128)
        col_full = sum_over(columns[matrix], "row", n_row)
        old_rows = row_moment[matrix].reshape(rows // 128, 128)
        old_cols = col_moment[matrix].reshape(1, width)
        return (
            second_decay * old_rows + (1.0 - second_decay) * row_full / total_cols,
            second_decay * old_cols + (1.0 - second_decay) * col_full / total_rows,
        )

    for slot in range(len(chunks) + bits + 1):
        if slot < len(chunks):
            sent = peer_half(table, terms, token, chunks[slot], places, width)
            token = sent
            from_peer[slot] = exchange(sent, "col", n_col, 1)
        for stage in range(bits):
            i = slot - 1 - stage
            if not 0 <= i < len(chunks):
                continue
            base = places >> (stage + 1)
            sums = partial_sums(
                table, terms, from_peer[i], received[i], token, chunks[i], base, width
            )
            token = sums[0]
            received[i].append(
                [
                    exchange(sums[half], "col", n_col, 2 << orders[half][stage])
                    for half in range(2)
                ]
            )
        if pending:
            pending.pop(0)()
        i = slot - 1 - bits
        if i < 0:
            continue
        matrix = chunks[i][0]
        gradient[matrix], row_part, columns[matrix] = final_sums(
            table, terms, from_peer[i], received[i], gradient[matrix], columns[matrix],
            token, chunks[i], half_rows, width,
        )
        token = columns[matrix]
        row_sums[matrix].append(row_part)
        if i != last_of[matrix]:
            continue

        state = {}

        def moments(matrix=matrix, state=state):
            nonlocal token
            r, c = statistics(matrix)
            new_rows[matrix], new_cols[matrix] = r, c
            state["g"] = gradient[matrix].reshape(rows, width)
            state["r"], state["c"] = lax.rsqrt(r), lax.rsqrt(c)
            state["lanes"] = clip_lanes(state["g"], state["r"], state["c"], token, width)
            token = state["lanes"]

        def finish(matrix=matrix, state=state):
            nonlocal token, output
            both = jnp.concatenate(
                [state["lanes"], jnp.sum(new_rows[matrix], axis=0, keepdims=True)], axis=0
            )
            both = jnp.sum(sum_over(sum_over(both, "col", n_col), "row", n_row), axis=1)
            row_level = both[1] / n_col / total_rows
            clip = jnp.maximum(
                1.0, jnp.sqrt(both[0] * row_level / (total_rows * total_cols))
            )
            col_factor = state["c"] * (jnp.sqrt(row_level) / clip)
            output = scale(
                state["g"], state["r"], col_factor, output, token, matrix, mats, width
            )
            token = output

        if i == len(chunks) - 1:
            moments()
            finish()
        else:
            pending += [moments, finish]

    return (
        output,
        jnp.stack([r.reshape(rows) for r in new_rows]),
        jnp.concatenate(new_cols, axis=0),
    )


def solution(mesh):
    placed = (P("col", None, "row", None), P(None, "row"), P(None, "col"))
    return jax.shard_map(
        functools.partial(on_device, mesh.shape["row"], mesh.shape["col"]),
        mesh=mesh,
        in_specs=placed,
        out_specs=(P(None, "row", "col"), P(None, "row"), P(None, "col")),
        check_vma=False,
    )
```

```python
import jax
import jax.numpy as jnp
from jax import lax
from jax.experimental import pallas as pl
from jax.experimental.pallas import tpu as pltpu
from jax.sharding import PartitionSpec as P


second_decay = 1.0 - 100.0 ** (-0.8)
tiny_square = 1e-30


FIRST = (1, 3, 4, 4, 4)
LAST = (4, 4, 4, 2, 2)
LANES = 128
STEP = 64

ANY = pl.BlockSpec(memory_space=pl.ANY)
ON_CHIP = pl.BlockSpec(memory_space=pltpu.VMEM)
LIMITS = pltpu.CompilerParams(vmem_limit_bytes=24 << 20)


def on_chip(value):
    return pltpu.with_memory_space_constraint(value, pltpu.VMEM)


def in_hbm(value):
    return pltpu.with_memory_space_constraint(value, pltpu.HBM)


def hbm_shape(shape):
    return pltpu.HBM(shape, jnp.float32)


def exchange(value, axis, size, mask):
    return lax.ppermute(value, axis, [(i, i ^ mask) for i in range(size)])


def chip_shape(shape):
    return pltpu.VMEM(shape, jnp.float32)


def added(refs):
    total = refs[0][...]
    for ref in refs[1:]:
        total = total + ref[...]
    return total


def add(parts):
    def body(*refs):
        refs[-1][...] = added(refs[:-1])

    return pl.pallas_call(
        body,
        in_specs=[ON_CHIP] * len(parts),
        out_specs=ON_CHIP,
        out_shape=chip_shape(parts[0].shape),
        compiler_params=LIMITS,
        name="add",
    )(*[on_chip(part) for part in parts])


def sum_over(value, axis, size):
    parts = [value]
    mask = 1
    while mask < size:
        value = parts[0] if len(parts) == 1 else add(parts)
        parts = [value, exchange(value, axis, size, mask)]
        mask *= 2
    return parts


def block_of(start, rows, most):
    return max(
        b for b in range(16, most + 1, 16) if b == 16 or not (rows % b or start % b)
    )


def peer_half(table, terms, token, chunk, places, width):
    matrix, start, rows = chunk
    block = block_of(start, rows, STEP)

    def body(table_ref, *refs):
        out = refs[-1]
        for half in range(2):
            for p in range(places):
                out[half, p] = refs[half * places + p][...].astype(jnp.float32)

    def terms_spec(half, p):
        return pl.BlockSpec(
            (None, None, block, width),
            lambda i, t: (matrix, half, start // block + i, t[half, p] ^ 1),
        )

    specs = [terms_spec(half, p) for half in range(2) for p in range(places)]
    return pl.pallas_call(
        body,
        grid_spec=pltpu.PrefetchScalarGridSpec(
            num_scalar_prefetch=1,
            grid=(rows // block,),
            in_specs=[*specs, ANY],
            out_specs=pl.BlockSpec((2, places, block, width), lambda i, t: (0, 0, i, 0)),
        ),
        out_shape=hbm_shape((2, places, rows, width)),
        compiler_params=LIMITS,
        name="peer_half",
    )(table, *[terms] * len(specs), token)


def partial_sums(table, terms, from_peer, received, token, chunk, base, width):
    matrix, start, rows = chunk
    block = block_of(start, rows, STEP)
    count = len(received)

    def body(table_ref, *refs):
        own, refs = refs[: 2 * base], refs[2 * base :]
        peer, others, outs = refs[0], refs[1 : 1 + 2 * count], refs[-2:]
        for half in range(2):
            for p in range(base):
                total = own[half * base + p][...].astype(jnp.float32) + peer[half, p]
                for k in range(count):
                    total = total + others[2 * k + half][p]
                outs[half][p] = total

    def terms_spec(half, p):
        return pl.BlockSpec(
            (None, None, block, width),
            lambda i, t: (matrix, half, start // block + i, t[half, base + p]),
        )

    specs = [terms_spec(half, p) for half in range(2) for p in range(base)]
    shifted = pl.BlockSpec((base, block, width), lambda i, t: (1, i, 0))
    plain = pl.BlockSpec((base, block, width), lambda i, t: (0, i, 0))
    shape = hbm_shape((base, rows, width))
    return pl.pallas_call(
        body,
        grid_spec=pltpu.PrefetchScalarGridSpec(
            num_scalar_prefetch=1,
            grid=(rows // block,),
            in_specs=[
                *specs,
                pl.BlockSpec((2, base, block, width), lambda i, t: (0, 1, i, 0)),
                *[shifted] * (2 * count),
                ANY,
            ],
            out_specs=[plain, plain],
        ),
        out_shape=[shape, shape],
        compiler_params=LIMITS,
        name="partial_sums",
    )(
        table, *[terms] * len(specs), in_hbm(from_peer),
        *[in_hbm(r) for pair in received for r in pair], token,
    )


def lane_groups(values, width):
    total = values[:, :LANES]
    for c in range(LANES, width, LANES):
        total = total + values[:, c : c + LANES]
    return total


def final_sums(table, terms, from_peer, received, totals, token, chunk, half_rows, width):
    matrix, start, rows = chunk
    block = block_of(start, rows, STEP)
    steps = rows // block
    count = len(received)
    begin = totals is None

    def body(table_ref, own, peer, *refs):
        others = refs[: 2 * count]
        out, row_out, col_out, lanes = refs[-4:]
        i = pl.program_id(0)

        @pl.when(i == 0)
        def _():
            if begin:
                col_out[...] = jnp.zeros_like(col_out)

        for half in range(2):
            total = own[half].astype(jnp.float32) + peer[half]
            for k in range(count):
                total = total + others[2 * k + half][...]
            out[half, pl.ds(pl.multiple_of(start + i * block, 8), block), :] = total
            squares = total * total + tiny_square
            col_out[...] += jnp.sum(squares, axis=0, keepdims=True)
            lanes[half, pl.ds(pl.multiple_of(i * block, block), block), :] = lane_groups(
                squares, width
            )

        @pl.when(i == steps - 1)
        def _():
            for half in range(2):
                row_out[half : half + 1, start : start + rows] = jnp.sum(
                    lanes[half].T, axis=0, keepdims=True
                )

    one = pl.BlockSpec((None, block, width), lambda i, t: (0, i, 0))
    first = 3 + 2 * count
    return pl.pallas_call(
        body,
        grid_spec=pltpu.PrefetchScalarGridSpec(
            num_scalar_prefetch=1,
            grid=(steps,),
            in_specs=[
                pl.BlockSpec(
                    (None, 2, block, width),
                    lambda i, t: (matrix, 0, start // block + i, t[0, 0]),
                ),
                pl.BlockSpec((2, None, block, width), lambda i, t: (0, 0, i, 0)),
                *[one] * (2 * count),
                *([] if begin else [ON_CHIP] * 3),
                ANY,
            ],
            out_specs=[ON_CHIP] * 3,
            scratch_shapes=[pltpu.VMEM((2, rows, LANES), jnp.float32)],
        ),
        out_shape=[
            chip_shape((2, half_rows, width)),
            chip_shape((2, half_rows)),
            chip_shape((1, width)),
        ],
        input_output_aliases={} if begin else {first + k: k for k in range(3)},
        compiler_params=LIMITS,
        name="final_sums",
    )(
        table, terms, in_hbm(from_peer), *[in_hbm(r) for pair in received for r in pair],
        *([] if begin else [on_chip(v) for v in totals]), token,
    )


def down_rows(row):
    return jnp.broadcast_to(row, (LANES, LANES)).T


def over_rows(gradient, row_parts, columns, row_moment, so_far, token, matrix, sizes):
    mats, rows, width, total_cols = sizes
    half_rows = rows // 2
    count = len(row_parts)
    begin = so_far is None

    def body(g, *refs):
        parts, (col, old) = refs[:count], refs[count : count + 2]
        out, moments, message = refs[-3:]
        if begin:
            message[...] = jnp.zeros_like(message)
        message[matrix : matrix + 1, :] = col[...]
        level = jnp.zeros((1, LANES), jnp.float32)
        squares = [jnp.zeros((8, LANES), jnp.float32)] * (width // LANES)
        for b in range(rows // LANES):
            half, first = b * LANES // half_rows, b * LANES % half_rows
            at = slice(first, first + LANES)
            total = parts[0][half : half + 1, at]
            for part in parts[1:]:
                total = total + part[half : half + 1, at]
            whole = slice(b * LANES, (b + 1) * LANES)
            moment = (
                second_decay * old[matrix : matrix + 1, whole]
                + (1.0 - second_decay) * total / total_cols
            )
            moments[matrix : matrix + 1, whole] = moment
            level = level + moment
            factor = down_rows(lax.rsqrt(moment))
            for k in range(width // LANES):
                lane = slice(k * LANES, (k + 1) * LANES)
                scaled = g[half, at, lane] * factor
                out[half, at, lane] = scaled
                squares[k] = squares[k] + jnp.sum(
                    (scaled * scaled).reshape(LANES // 8, 8, LANES), axis=0
                )
        for k in range(width // LANES):
            message[mats + matrix : mats + matrix + 1, k * LANES : (k + 1) * LANES] = jnp.sum(
                squares[k], axis=0, keepdims=True
            )
        message[2 * mats + matrix : 2 * mats + matrix + 1, :LANES] = level

    return pl.pallas_call(
        body,
        in_specs=[ON_CHIP] * (3 + count + (0 if begin else 2)) + [ANY],
        out_specs=[ON_CHIP] * 3,
        out_shape=[
            chip_shape(gradient.shape),
            chip_shape((mats, rows)),
            chip_shape((3 * mats, width)),
        ],
        input_output_aliases={0: 0} if begin else {0: 0, 3 + count: 1, 4 + count: 2},
        compiler_params=LIMITS,
        name="over_rows",
    )(
        *[on_chip(v) for v in (gradient, *row_parts, columns, row_moment)],
        *([] if begin else [on_chip(v) for v in so_far]), token,
    )


def over_columns(parts, col_moment, sizes, total_rows):
    mats, _, width, _ = sizes

    def body(*refs):
        old, new_cols, levels, lanes = refs[len(parts) :]
        both = added(refs[: len(parts)])
        new = second_decay * old[...] + (1.0 - second_decay) * both[:mats] / total_rows
        new_cols[...] = new
        lanes[...] = lane_groups(both[mats : 2 * mats] / new, width)
        levels[...] = jnp.broadcast_to(
            jnp.sum(both[2 * mats :], axis=1, keepdims=True) / total_rows, (mats, LANES)
        )

    return pl.pallas_call(
        body,
        in_specs=[ON_CHIP] * (len(parts) + 1),
        out_specs=[ON_CHIP] * 3,
        out_shape=[
            chip_shape((mats, width)), chip_shape((mats, LANES)), chip_shape((mats, LANES)),
        ],
        compiler_params=LIMITS,
        name="over_columns",
    )(*[on_chip(v) for v in (*parts, col_moment)])


def scale(scaled, new_rows, new_cols, levels, clip_parts, sizes, total_rows):
    mats, rows, width, total_cols = sizes
    half_rows = rows // 2
    block = half_rows // 2
    count = len(clip_parts)

    def body(*refs):
        r, c, level, *parts = refs[mats : mats + 3 + count]
        out, rows_out, cols_out = refs[-3:]
        m, i = pl.program_id(0), pl.program_id(1)

        @pl.when((m == 0) & (i == 0))
        def _():
            rows_out[...] = r[...]
            cols_out[...] = c[...]

        for matrix in range(mats):

            @pl.when(m == matrix)
            def _(matrix=matrix):
                one = slice(matrix, matrix + 1)
                row_level = level[one, :1]
                clip = parts[0][one, :]
                for part in parts[1:]:
                    clip = clip + part[one, :]
                clip = jnp.sum(clip, axis=1, keepdims=True)
                clip = jnp.sqrt(clip * row_level / (total_rows * total_cols))
                factor = lax.rsqrt(c[one, :]) * (jnp.sqrt(row_level) / jnp.maximum(1.0, clip))
                at = pl.ds(pl.multiple_of((i % 2) * block, 8), block)
                out[...] = refs[matrix][i // 2, at, :] * factor

    return pl.pallas_call(
        body,
        grid=(mats, 4),
        in_specs=[ON_CHIP] * (mats + 3 + count),
        out_specs=[
            pl.BlockSpec((None, block, width), lambda m, i: (m, i, 0)),
            pl.BlockSpec((mats, rows), lambda m, i: (0, 0)),
            pl.BlockSpec((mats, width), lambda m, i: (0, 0)),
        ],
        out_shape=[hbm_shape((mats, rows, width)), hbm_shape((mats, rows)), hbm_shape((mats, width))],
        compiler_params=LIMITS,
        name="scale",
    )(*[on_chip(v) for v in (*scaled, new_rows, new_cols, levels, *clip_parts)])


def chunks_of(mats):
    chunks = []
    for matrix in range(mats):
        start = 0
        for size in LAST if matrix == mats - 1 else FIRST:
            chunks.append((matrix, start, size))
            start += size
    return chunks


def kernel_order(count, bits):
    order = [("peer", 0), ("peer", 1)]
    for t in range(-2, count + max(bits, 1)):
        step = [(f"sum{k}", t - k + 1) for k in range(1, bits)]
        step += [("final", t - max(bits - 1, 0))]
        step += [("sum0", t + 2)] if bits else []
        step += [("peer", t + 3)]
        order += [
            (stage, i) for stage, i in step if 0 <= i < count and (stage, i) not in order
        ]
    return order


def on_device(n_row, n_col, grad_terms, row_moment, col_moment):
    _, mats, rows, all_width = grad_terms.shape
    width = all_width // n_col
    half_rows = rows // 2
    bits = n_col.bit_length() - 2
    places = 1 << bits
    total_rows, total_cols = rows * n_row, all_width
    sizes = (mats, rows, width, total_cols)

    me = lax.axis_index("col").astype(jnp.int32)
    terms = grad_terms.reshape(mats, 2, half_rows, all_width)
    orders = (tuple(range(bits)), tuple(reversed(range(bits))))

    def place_mask(order, place):
        return sum(1 << bit for k, bit in enumerate(order) if place >> (bits - 1 - k) & 1)

    masks = [[2 * place_mask(order, p) for p in range(places)] for order in orders]
    table = jnp.bitwise_xor(jnp.array(masks, jnp.int32), me)

    unit = half_rows // 16
    chunks = [(m, start * unit, size * unit) for m, start, size in chunks_of(mats)]
    last_of = {c[0]: i for i, c in enumerate(chunks)}

    from_peer, received = {}, {i: [] for i in range(len(chunks))}
    totals, row_parts, scaled = [None] * mats, [None] * mats, [None] * mats
    so_far = None
    token = in_hbm(terms)

    def divide_rows(matrix):
        nonlocal so_far, token
        gradient, _, columns = totals[matrix]
        scaled[matrix], *so_far = over_rows(
            gradient, row_parts[matrix], columns, row_moment, so_far, token, matrix, sizes
        )
        token = on_chip(so_far[1])

    finished = []
    for stage, i in kernel_order(len(chunks), bits):
        for entry in finished:
            entry[1] -= 1
            if entry[1] == 0:
                divide_rows(entry[0])
        matrix = chunks[i][0]
        if stage == "peer":
            sent = peer_half(table, terms, token, chunks[i], places, width)
        elif stage == "final":
            totals[matrix] = final_sums(
                table, terms, from_peer[i], received[i], totals[matrix], token,
                chunks[i], half_rows, width,
            )
        else:
            k = int(stage[3:])
            sums = partial_sums(
                table, terms, from_peer[i], received[i], token, chunks[i],
                places >> (k + 1), width,
            )
        if stage == "peer":
            token = in_hbm(sent)
            from_peer[i] = exchange(sent, "col", n_col, 1)
        elif stage == "final":
            token = on_chip(totals[matrix][2])
            if i == last_of[matrix]:
                row_parts[matrix] = sum_over(totals[matrix][1], "col", n_col)
                finished.append([matrix, 4 * n_col.bit_length() - 5])
        else:
            token = in_hbm(sums[0])
            received[i].append(
                [exchange(sums[half], "col", n_col, 2 << orders[half][k]) for half in range(2)]
            )
    for matrix in range(mats):
        if scaled[matrix] is None:
            divide_rows(matrix)

    new_rows, message = so_far
    new_cols, levels, lanes = over_columns(
        sum_over(message, "row", n_row), col_moment, sizes, total_rows
    )
    clip_parts = sum_over(lanes, "col", n_col)
    return scale(scaled, new_rows, new_cols, levels, clip_parts, sizes, total_rows)


def solution(mesh):
    n_row, n_col = mesh.shape["row"], mesh.shape["col"]
    placed = (P("col", None, "row", None), P(None, "row"), P(None, "col"))

    def body(*args):
        return on_device(n_row, n_col, *args)

    return jax.shard_map(
        body,
        mesh=mesh,
        in_specs=placed,
        out_specs=(P(None, "row", "col"), P(None, "row"), P(None, "col")),
        check_vma=False,
    )
```

```python
import jax
import jax.numpy as jnp
from jax import lax
from jax.experimental import pallas as pl
from jax.experimental.pallas import tpu as pltpu
from jax.sharding import PartitionSpec as P


second_decay = 1.0 - 100.0 ** (-0.8)
tiny_square = 1e-30


FIRST = (1, 3, 4, 4, 4)
LAST = (4, 4, 4, 2, 2)
LANES = 128
ON_CHIP_CHUNKS = (0, 1, -1)
STEP = 64

ANY = pl.BlockSpec(memory_space=pl.ANY)
ON_CHIP = pl.BlockSpec(memory_space=pltpu.VMEM)
LIMITS = pltpu.CompilerParams(vmem_limit_bytes=24 << 20)


def on_chip(value):
    return pltpu.with_memory_space_constraint(value, pltpu.VMEM)


def in_hbm(value):
    return pltpu.with_memory_space_constraint(value, pltpu.HBM)


def hbm_shape(shape):
    return pltpu.HBM(shape, jnp.float32)


def exchange(value, axis, size, mask):
    return lax.ppermute(value, axis, [(i, i ^ mask) for i in range(size)])


def chip_shape(shape):
    return pltpu.VMEM(shape, jnp.float32)


def added(values):
    values = list(values)
    while len(values) > 1:
        values = [a + b for a, b in zip(values[::2], values[1::2])]
    return values[0]


def add(parts):
    def body(*refs):
        refs[-1][...] = added(ref[...] for ref in refs[:-1])

    return pl.pallas_call(
        body,
        in_specs=[ON_CHIP] * len(parts),
        out_specs=ON_CHIP,
        out_shape=chip_shape(parts[0].shape),
        compiler_params=LIMITS,
        name="add",
    )(*[on_chip(part) for part in parts])


def rounds_of(size):
    bits = size.bit_length() - 1
    rounds = [(1,)] if bits % 2 else []
    for low in range(bits % 2, bits, 2):
        rounds.append((1 << low, 2 << low, 3 << low))
    return rounds


def sum_over(value, axis, size):
    parts = [value]
    for masks in rounds_of(size):
        value = parts[0] if len(parts) == 1 else add(parts)
        parts = [value]
        parts += [exchange(value, axis, size, mask) for mask in masks]
    return parts


def block_of(start, rows, most):
    return max(
        b for b in range(16, most + 1, 16) if b == 16 or not (rows % b or start % b)
    )


def rows_at(block):
    return pl.ds(pl.multiple_of(pl.program_id(0) * block, 16), block)


def peer_half(table, terms, token, chunk, places, width, chip):
    matrix, start, rows = chunk
    block = block_of(start, rows, STEP)

    def body(table_ref, *refs):
        out = refs[-1]
        at = rows_at(block) if chip else slice(None)
        for half in range(2):
            for p in range(places):
                out[half, p, at] = refs[half * places + p][...].astype(jnp.float32)

    def terms_spec(half, p):
        return pl.BlockSpec(
            (None, None, block, width),
            lambda i, t: (matrix, half, start // block + i, t[half, p] ^ 1),
        )

    specs = [terms_spec(half, p) for half in range(2) for p in range(places)]
    return pl.pallas_call(
        body,
        grid_spec=pltpu.PrefetchScalarGridSpec(
            num_scalar_prefetch=1,
            grid=(rows // block,),
            in_specs=[*specs, ANY],
            out_specs=ON_CHIP
            if chip
            else pl.BlockSpec((2, places, block, width), lambda i, t: (0, 0, i, 0)),
        ),
        out_shape=(chip_shape if chip else hbm_shape)((2, places, rows, width)),
        compiler_params=LIMITS,
        name="peer_half",
    )(table, *[terms] * len(specs), token)


def partial_sums(table, terms, from_peer, received, token, chunk, base, width, chip):
    matrix, start, rows = chunk
    block = block_of(start, rows, STEP)
    count = len(received)

    def body(table_ref, *refs):
        own, refs = refs[: 2 * base], refs[2 * base :]
        peer, others, outs = refs[0], refs[1 : 1 + 2 * count], refs[-2:]
        first, at = (base, rows_at(block)) if chip else (0, slice(None))
        for half in range(2):
            for p in range(base):
                total = own[half * base + p][...].astype(jnp.float32)
                total = total + peer[half, first + p, at]
                for k in range(count):
                    total = total + others[2 * k + half][first + p, at]
                outs[half][p, at] = total

    def terms_spec(half, p):
        return pl.BlockSpec(
            (None, None, block, width),
            lambda i, t: (matrix, half, start // block + i, t[half, base + p]),
        )

    specs = [terms_spec(half, p) for half in range(2) for p in range(base)]
    of_peer = pl.BlockSpec((2, base, block, width), lambda i, t: (0, 1, i, 0))
    shifted = pl.BlockSpec((base, block, width), lambda i, t: (1, i, 0))
    plain = pl.BlockSpec((base, block, width), lambda i, t: (0, i, 0))
    if chip:
        of_peer = shifted = plain = ON_CHIP
    shape = (chip_shape if chip else hbm_shape)((base, rows, width))
    put = on_chip if chip else in_hbm
    return pl.pallas_call(
        body,
        grid_spec=pltpu.PrefetchScalarGridSpec(
            num_scalar_prefetch=1,
            grid=(rows // block,),
            in_specs=[
                *specs,
                of_peer,
                *[shifted] * (2 * count),
                ANY,
            ],
            out_specs=[plain, plain],
        ),
        out_shape=[shape, shape],
        compiler_params=LIMITS,
        name="partial_sums",
    )(
        table, *[terms] * len(specs), put(from_peer),
        *[put(r) for pair in received for r in pair], token,
    )


def lane_groups(values, width):
    total = values[:, :LANES]
    for c in range(LANES, width, LANES):
        total = total + values[:, c : c + LANES]
    return total


def final_sums(table, terms, from_peer, received, totals, token, chunk, half_rows, width, chip):
    matrix, start, rows = chunk
    block = block_of(start, rows, STEP)
    steps = rows // block
    count = len(received)
    begin = totals is None

    def body(table_ref, own, peer, *refs):
        others = refs[: 2 * count]
        out, row_out, col_out, lanes = refs[-4:]
        i = pl.program_id(0)

        @pl.when(i == 0)
        def _():
            if begin:
                col_out[...] = jnp.zeros_like(col_out)

        for half in range(2):
            total = own[half].astype(jnp.float32)
            if chip:
                total = total + peer[half, 0, rows_at(block)]
            else:
                total = total + peer[half]
            for k in range(count):
                other = others[2 * k + half]
                total = total + (other[0, rows_at(block)] if chip else other[...])
            out[half, pl.ds(pl.multiple_of(start + i * block, 8), block), :] = total
            squares = total * total + tiny_square
            col_out[...] += jnp.sum(squares, axis=0, keepdims=True)
            lanes[half, pl.ds(pl.multiple_of(i * block, block), block), :] = lane_groups(
                squares, width
            )

        @pl.when(i == steps - 1)
        def _():
            for half in range(2):
                row_out[half : half + 1, start : start + rows] = jnp.sum(
                    lanes[half].T, axis=0, keepdims=True
                )

    of_peer = pl.BlockSpec((2, None, block, width), lambda i, t: (0, 0, i, 0))
    one = pl.BlockSpec((None, block, width), lambda i, t: (0, i, 0))
    if chip:
        of_peer = one = ON_CHIP
    put = on_chip if chip else in_hbm
    first = 3 + 2 * count
    return pl.pallas_call(
        body,
        grid_spec=pltpu.PrefetchScalarGridSpec(
            num_scalar_prefetch=1,
            grid=(steps,),
            in_specs=[
                pl.BlockSpec(
                    (None, 2, block, width),
                    lambda i, t: (matrix, 0, start // block + i, t[0, 0]),
                ),
                of_peer,
                *[one] * (2 * count),
                *([] if begin else [ON_CHIP] * 3),
                ANY,
            ],
            out_specs=[ON_CHIP] * 3,
            scratch_shapes=[pltpu.VMEM((2, rows, LANES), jnp.float32)],
        ),
        out_shape=[
            chip_shape((2, half_rows, width)),
            chip_shape((2, half_rows)),
            chip_shape((1, width)),
        ],
        input_output_aliases={} if begin else {first + k: k for k in range(3)},
        compiler_params=LIMITS,
        name="final_sums",
    )(
        table, terms, put(from_peer), *[put(r) for pair in received for r in pair],
        *([] if begin else [on_chip(v) for v in totals]), token,
    )


def down_rows(row):
    return jnp.broadcast_to(row, (LANES, LANES)).T


def over_rows(gradient, row_parts, columns, row_moment, new_rows, token, matrix, sizes):
    mats, rows, width, total_cols = sizes
    half_rows = rows // 2
    count = len(row_parts)
    begin = new_rows is None

    def body(g, *refs):
        parts, (col, old) = refs[:count], refs[count : count + 2]
        out, moments, message = refs[-3:]
        level = jnp.zeros((1, LANES), jnp.float32)
        squares = [jnp.zeros((8, LANES), jnp.float32)] * (width // LANES)
        for b in range(rows // LANES):
            half, first = b * LANES // half_rows, b * LANES % half_rows
            at = slice(first, first + LANES)
            total = added(part[half : half + 1, at] for part in parts)
            whole = slice(b * LANES, (b + 1) * LANES)
            moment = (
                second_decay * old[matrix : matrix + 1, whole]
                + (1.0 - second_decay) * total / total_cols
            )
            moments[matrix : matrix + 1, whole] = moment
            level = level + moment
            factor = down_rows(lax.rsqrt(moment))
            for k in range(width // LANES):
                lane = slice(k * LANES, (k + 1) * LANES)
                value = g[half, at, lane] * factor
                out[half, at, lane] = value
                squares[k] = squares[k] + jnp.sum(
                    (value * value).reshape(LANES // 8, 8, LANES), axis=0
                )
        message[0:1, :width] = col[...]
        message[0:1, width:] = level
        for k in range(width // LANES):
            message[1:2, k * LANES : (k + 1) * LANES] = jnp.sum(
                squares[k], axis=0, keepdims=True
            )
        message[1:2, width:] = jnp.zeros_like(level)

    return pl.pallas_call(
        body,
        in_specs=[ON_CHIP] * (3 + count + (0 if begin else 1)) + [ANY],
        out_specs=[ON_CHIP] * 3,
        out_shape=[
            chip_shape(gradient.shape),
            chip_shape((mats, rows)),
            chip_shape((2, width + LANES)),
        ],
        input_output_aliases={0: 0} if begin else {0: 0, 3 + count: 1},
        compiler_params=LIMITS,
        name="over_rows",
    )(
        *[on_chip(v) for v in (gradient, *row_parts, columns, row_moment)],
        *([] if begin else [on_chip(new_rows)]), token,
    )


def over_columns(messages, col_moment, sizes, total_rows):
    mats, _, width, _ = sizes
    count = len(messages[0])

    def body(*refs):
        old, new_cols, levels, lanes = refs[mats * count :]
        for matrix in range(mats):
            one = slice(matrix, matrix + 1)
            both = added(
                part[...] for part in refs[matrix * count : (matrix + 1) * count]
            )
            new = (
                second_decay * old[one, :]
                + (1.0 - second_decay) * both[0:1, :width] / total_rows
            )
            new_cols[one, :] = new
            lanes[one, :] = lane_groups(both[1:2, :width] / new, width)
            level = jnp.sum(both[0:1, width:], axis=1, keepdims=True) / total_rows
            levels[one, :] = jnp.broadcast_to(level, (1, LANES))

    return pl.pallas_call(
        body,
        in_specs=[ON_CHIP] * (mats * count + 1),
        out_specs=[ON_CHIP] * 3,
        out_shape=[
            chip_shape((mats, width)), chip_shape((mats, LANES)), chip_shape((mats, LANES)),
        ],
        compiler_params=LIMITS,
        name="over_columns",
    )(*[on_chip(v) for parts in messages for v in parts], on_chip(col_moment))


def scale(scaled, new_cols, levels, clip_parts, sizes, total_rows):
    mats, rows, width, total_cols = sizes
    half_rows = rows // 2
    pieces = 4
    piece = half_rows // pieces
    count = len(clip_parts)

    def body(*refs):
        c, level, *parts = refs[mats : mats + 2 + count]
        out, ready, sent = refs[-3:]

        def copy(matrix, half, k):
            at = pl.ds(half * half_rows + k * piece, piece)
            return pltpu.make_async_copy(
                ready.at[matrix, at], out.at[matrix, at], sent.at[matrix, half * pieces + k]
            )

        places = [
            (matrix, half, k)
            for matrix in range(mats) for half in range(2) for k in range(pieces)
        ]
        for matrix, half, k in places:
            one = slice(matrix, matrix + 1)
            if half == k == 0:
                row_level = level[one, :1]
                clip = jnp.sum(added(p[one, :] for p in parts), axis=1, keepdims=True)
                clip = jnp.sqrt(clip * row_level / (total_rows * total_cols))
                factor = lax.rsqrt(c[one, :]) * (jnp.sqrt(row_level) / jnp.maximum(1.0, clip))
            at = slice(k * piece, (k + 1) * piece)
            to = slice(half * half_rows + k * piece, half * half_rows + (k + 1) * piece)
            ready[matrix, to, :] = refs[matrix][half, at, :] * factor
            copy(matrix, half, k).start()
        for place in places:
            copy(*place).wait()

    return pl.pallas_call(
        body,
        in_specs=[ON_CHIP] * (mats + 2 + count),
        out_specs=ANY,
        out_shape=hbm_shape((mats, rows, width)),
        scratch_shapes=[
            pltpu.VMEM((mats, rows, width), jnp.float32),
            pltpu.SemaphoreType.DMA((mats, 2 * pieces)),
        ],
        compiler_params=LIMITS,
        name="scale",
    )(*[on_chip(v) for v in (*scaled, new_cols, levels, *clip_parts)])


def chunks_of(mats):
    chunks = []
    for matrix in range(mats):
        start = 0
        for size in LAST if matrix == mats - 1 else FIRST:
            chunks.append((matrix, start, size))
            start += size
    return chunks


def kernel_order(count, bits):
    order = [("peer", 0), ("peer", 1)]
    for t in range(-2, count + max(bits, 1)):
        step = [(f"sum{k}", t - k + 1) for k in range(1, bits)]
        step += [("final", t - max(bits - 1, 0))]
        step += [("sum0", t + 2)] if bits else []
        step += [("peer", t + 3)]
        order += [
            (stage, i) for stage, i in step if 0 <= i < count and (stage, i) not in order
        ]
    return order


def rounds_after(n_col):
    return 6 * len(rounds_of(n_col)) - 3


def on_device(n_row, n_col, grad_terms, row_moment, col_moment):
    _, mats, rows, all_width = grad_terms.shape
    width = all_width // n_col
    half_rows = rows // 2
    bits = n_col.bit_length() - 2
    places = 1 << bits
    total_rows, total_cols = rows * n_row, all_width
    sizes = (mats, rows, width, total_cols)

    me = lax.axis_index("col").astype(jnp.int32)
    terms = grad_terms.reshape(mats, 2, half_rows, all_width)
    orders = (tuple(range(bits)), tuple(reversed(range(bits))))

    def place_mask(order, place):
        return sum(1 << bit for k, bit in enumerate(order) if place >> (bits - 1 - k) & 1)

    masks = [[2 * place_mask(order, p) for p in range(places)] for order in orders]
    table = jnp.bitwise_xor(jnp.array(masks, jnp.int32), me)

    unit = half_rows // 16
    chunks = [(m, start * unit, size * unit) for m, start, size in chunks_of(mats)]
    last_of = {c[0]: i for i, c in enumerate(chunks)}

    from_peer, received = {}, {i: [] for i in range(len(chunks))}
    totals, row_parts, scaled = [None] * mats, [None] * mats, [None] * mats
    messages, new_rows = [None] * mats, None
    token = in_hbm(terms)

    def divide_rows(matrix):
        nonlocal new_rows, token
        gradient, _, columns = totals[matrix]
        scaled[matrix], new_rows, message = over_rows(
            gradient, row_parts[matrix], columns, row_moment, new_rows, token, matrix, sizes
        )
        token = on_chip(message)
        messages[matrix] = sum_over(message, "row", n_row)

    finished = []
    for stage, i in kernel_order(len(chunks), bits):
        for entry in finished:
            entry[1] -= 1
            if entry[1] == 0:
                divide_rows(entry[0])
        matrix = chunks[i][0]
        chip = i in ON_CHIP_CHUNKS or i - len(chunks) in ON_CHIP_CHUNKS
        put = on_chip if chip else in_hbm
        if stage == "peer":
            sent = peer_half(table, terms, token, chunks[i], places, width, chip)
        elif stage == "final":
            totals[matrix] = final_sums(
                table, terms, from_peer[i], received[i], totals[matrix], token,
                chunks[i], half_rows, width, chip,
            )
        else:
            k = int(stage[3:])
            sums = partial_sums(
                table, terms, from_peer[i], received[i], token, chunks[i],
                places >> (k + 1), width, chip,
            )
        if stage == "peer":
            token = put(sent)
            from_peer[i] = exchange(sent, "col", n_col, 1)
        elif stage == "final":
            token = on_chip(totals[matrix][2])
            if i == last_of[matrix]:
                row_parts[matrix] = sum_over(totals[matrix][1], "col", n_col)
                finished.append([matrix, rounds_after(n_col)])
        else:
            token = put(sums[0])
            received[i].append(
                [exchange(sums[half], "col", n_col, 2 << orders[half][k]) for half in range(2)]
            )
    for matrix in range(mats):
        if scaled[matrix] is None:
            divide_rows(matrix)

    new_cols, levels, lanes = over_columns(messages, col_moment, sizes, total_rows)
    clip_parts = sum_over(lanes, "col", n_col)
    update = scale(scaled, new_cols, levels, clip_parts, sizes, total_rows)
    return update, new_rows, new_cols


def solution(mesh):
    n_row, n_col = mesh.shape["row"], mesh.shape["col"]
    placed = (P("col", None, "row", None), P(None, "row"), P(None, "col"))

    def body(*args):
        return on_device(n_row, n_col, *args)

    return jax.shard_map(
        body,
        mesh=mesh,
        in_specs=placed,
        out_specs=(P(None, "row", "col"), P(None, "row"), P(None, "col")),
        check_vma=False,
    )
```

```python
import jax
import jax.numpy as jnp
from jax import lax
from jax.experimental import pallas as pl
from jax.experimental.pallas import tpu as pltpu
from jax.sharding import PartitionSpec as P


second_decay = 1.0 - 100.0 ** (-0.8)
tiny_square = 1e-30


FIRST = (1, 3, 4, 4, 4)
LAST = (4, 4, 4, 2, 2)
LANES = 128
ON_CHIP_CHUNKS = (0, 1, -1)
STEP = 64

ANY = pl.BlockSpec(memory_space=pl.ANY)
ON_CHIP = pl.BlockSpec(memory_space=pltpu.VMEM)
LIMITS = pltpu.CompilerParams(vmem_limit_bytes=24 << 20)


def on_chip(value):
    return pltpu.with_memory_space_constraint(value, pltpu.VMEM)


def in_hbm(value):
    return pltpu.with_memory_space_constraint(value, pltpu.HBM)


def hbm_shape(shape):
    return pltpu.HBM(shape, jnp.float32)


def exchange(value, axis, size, mask):
    return lax.ppermute(value, axis, [(i, i ^ mask) for i in range(size)])


def chip_shape(shape):
    return pltpu.VMEM(shape, jnp.float32)


def added(values):
    values = list(values)
    while len(values) > 1:
        values = [a + b for a, b in zip(values[::2], values[1::2])]
    return values[0]


def add(parts):
    def body(*refs):
        refs[-1][...] = added(ref[...] for ref in refs[:-1])

    return pl.pallas_call(
        body,
        in_specs=[ON_CHIP] * len(parts),
        out_specs=ON_CHIP,
        out_shape=chip_shape(parts[0].shape),
        compiler_params=LIMITS,
        name="add",
    )(*[on_chip(part) for part in parts])


def rounds_of(size):
    bits = size.bit_length() - 1
    rounds = [(1,)] if bits % 2 else []
    for low in range(bits % 2, bits, 2):
        rounds.append((1 << low, 2 << low, 3 << low))
    return rounds


def sum_over(value, axis, size):
    parts = [value]
    for masks in rounds_of(size):
        value = parts[0] if len(parts) == 1 else add(parts)
        parts = [value]
        parts += [exchange(value, axis, size, mask) for mask in masks]
    return parts


def block_of(start, rows, most):
    return max(
        b for b in range(16, most + 1, 16) if b == 16 or not (rows % b or start % b)
    )


def rows_at(block):
    return pl.ds(pl.multiple_of(pl.program_id(0) * block, 16), block)


def peer_half(table, terms, token, chunk, places, width, chip):
    matrix, start, rows = chunk
    block = block_of(start, rows, STEP)

    def body(table_ref, *refs):
        out = refs[-1]
        at = rows_at(block) if chip else slice(None)
        for half in range(2):
            for p in range(places):
                out[half, p, at] = refs[half * places + p][...].astype(jnp.float32)

    def terms_spec(half, p):
        return pl.BlockSpec(
            (None, None, block, width),
            lambda i, t: (matrix, half, start // block + i, t[half, p] ^ 1),
        )

    specs = [terms_spec(half, p) for half in range(2) for p in range(places)]
    return pl.pallas_call(
        body,
        grid_spec=pltpu.PrefetchScalarGridSpec(
            num_scalar_prefetch=1,
            grid=(rows // block,),
            in_specs=[*specs, ANY],
            out_specs=ON_CHIP
            if chip
            else pl.BlockSpec((2, places, block, width), lambda i, t: (0, 0, i, 0)),
        ),
        out_shape=(chip_shape if chip else hbm_shape)((2, places, rows, width)),
        compiler_params=LIMITS,
        name="peer_half",
    )(table, *[terms] * len(specs), token)


def partial_sums(table, terms, from_peer, received, token, chunk, base, width, chip):
    matrix, start, rows = chunk
    block = block_of(start, rows, STEP)
    count = len(received)

    def body(table_ref, *refs):
        own, refs = refs[: 2 * base], refs[2 * base :]
        peer, others, outs = refs[0], refs[1 : 1 + 2 * count], refs[-2:]
        first, at = (base, rows_at(block)) if chip else (0, slice(None))
        for half in range(2):
            for p in range(base):
                total = own[half * base + p][...].astype(jnp.float32)
                total = total + peer[half, first + p, at]
                for k in range(count):
                    total = total + others[2 * k + half][first + p, at]
                outs[half][p, at] = total

    def terms_spec(half, p):
        return pl.BlockSpec(
            (None, None, block, width),
            lambda i, t: (matrix, half, start // block + i, t[half, base + p]),
        )

    specs = [terms_spec(half, p) for half in range(2) for p in range(base)]
    of_peer = pl.BlockSpec((2, base, block, width), lambda i, t: (0, 1, i, 0))
    shifted = pl.BlockSpec((base, block, width), lambda i, t: (1, i, 0))
    plain = pl.BlockSpec((base, block, width), lambda i, t: (0, i, 0))
    if chip:
        of_peer = shifted = plain = ON_CHIP
    shape = (chip_shape if chip else hbm_shape)((base, rows, width))
    put = on_chip if chip else in_hbm
    return pl.pallas_call(
        body,
        grid_spec=pltpu.PrefetchScalarGridSpec(
            num_scalar_prefetch=1,
            grid=(rows // block,),
            in_specs=[
                *specs,
                of_peer,
                *[shifted] * (2 * count),
                ANY,
            ],
            out_specs=[plain, plain],
        ),
        out_shape=[shape, shape],
        compiler_params=LIMITS,
        name="partial_sums",
    )(
        table, *[terms] * len(specs), put(from_peer),
        *[put(r) for pair in received for r in pair], token,
    )


def lane_groups(values, width):
    total = values[:, :LANES]
    for c in range(LANES, width, LANES):
        total = total + values[:, c : c + LANES]
    return total


def final_sums(table, terms, from_peer, received, totals, token, chunk, half_rows, width, chip):
    matrix, start, rows = chunk
    block = block_of(start, rows, STEP)
    steps = rows // block
    count = len(received)
    begin = totals is None

    def body(table_ref, own, peer, *refs):
        others = refs[: 2 * count]
        out, row_out, col_out, lanes = refs[-4:]
        i = pl.program_id(0)

        @pl.when(i == 0)
        def _():
            if begin:
                col_out[...] = jnp.zeros_like(col_out)

        for half in range(2):
            total = own[half].astype(jnp.float32)
            if chip:
                total = total + peer[half, 0, rows_at(block)]
            else:
                total = total + peer[half]
            for k in range(count):
                other = others[2 * k + half]
                total = total + (other[0, rows_at(block)] if chip else other[...])
            out[half, pl.ds(pl.multiple_of(start + i * block, 8), block), :] = total
            squares = total * total + tiny_square
            col_out[...] += jnp.sum(squares, axis=0, keepdims=True)
            lanes[half, pl.ds(pl.multiple_of(i * block, block), block), :] = lane_groups(
                squares, width
            )

        @pl.when(i == steps - 1)
        def _():
            for half in range(2):
                row_out[half : half + 1, start : start + rows] = jnp.sum(
                    lanes[half].T, axis=0, keepdims=True
                )

    of_peer = pl.BlockSpec((2, None, block, width), lambda i, t: (0, 0, i, 0))
    one = pl.BlockSpec((None, block, width), lambda i, t: (0, i, 0))
    if chip:
        of_peer = one = ON_CHIP
    put = on_chip if chip else in_hbm
    first = 3 + 2 * count
    return pl.pallas_call(
        body,
        grid_spec=pltpu.PrefetchScalarGridSpec(
            num_scalar_prefetch=1,
            grid=(steps,),
            in_specs=[
                pl.BlockSpec(
                    (None, 2, block, width),
                    lambda i, t: (matrix, 0, start // block + i, t[0, 0]),
                ),
                of_peer,
                *[one] * (2 * count),
                *([] if begin else [ON_CHIP] * 3),
                ANY,
            ],
            out_specs=[ON_CHIP] * 3,
            scratch_shapes=[pltpu.VMEM((2, rows, LANES), jnp.float32)],
        ),
        out_shape=[
            chip_shape((2, half_rows, width)),
            chip_shape((2, half_rows)),
            chip_shape((1, width)),
        ],
        input_output_aliases={} if begin else {first + k: k for k in range(3)},
        compiler_params=LIMITS,
        name="final_sums",
    )(
        table, terms, put(from_peer), *[put(r) for pair in received for r in pair],
        *([] if begin else [on_chip(v) for v in totals]), token,
    )


def down_rows(row):
    return jnp.broadcast_to(row, (LANES, LANES)).T


def over_rows(gradient, row_parts, columns, row_moment, new_rows, token, matrix, sizes):
    mats, rows, width, total_cols = sizes
    half_rows = rows // 2
    count = len(row_parts)
    begin = new_rows is None

    def body(g, *refs):
        parts, (col, old) = refs[:count], refs[count : count + 2]
        out, moments, message = refs[-3:]
        level = jnp.zeros((1, LANES), jnp.float32)
        squares = [jnp.zeros((8, LANES), jnp.float32)] * (width // LANES)
        for b in range(rows // LANES):
            half, first = b * LANES // half_rows, b * LANES % half_rows
            at = slice(first, first + LANES)
            total = added(part[half : half + 1, at] for part in parts)
            whole = slice(b * LANES, (b + 1) * LANES)
            moment = (
                second_decay * old[matrix : matrix + 1, whole]
                + (1.0 - second_decay) * total / total_cols
            )
            moments[matrix : matrix + 1, whole] = moment
            level = level + moment
            factor = down_rows(lax.rsqrt(moment))
            for k in range(width // LANES):
                lane = slice(k * LANES, (k + 1) * LANES)
                value = g[half, at, lane] * factor
                out[half, at, lane] = value
                squares[k] = squares[k] + jnp.sum(
                    (value * value).reshape(LANES // 8, 8, LANES), axis=0
                )
        message[0:1, :width] = col[...]
        message[0:1, width:] = level
        for k in range(width // LANES):
            message[1:2, k * LANES : (k + 1) * LANES] = jnp.sum(
                squares[k], axis=0, keepdims=True
            )
        message[1:2, width:] = jnp.zeros_like(level)

    return pl.pallas_call(
        body,
        in_specs=[ON_CHIP] * (3 + count + (0 if begin else 1)) + [ANY],
        out_specs=[ON_CHIP] * 3,
        out_shape=[
            chip_shape(gradient.shape),
            chip_shape((mats, rows)),
            chip_shape((2, width + LANES)),
        ],
        input_output_aliases={0: 0} if begin else {0: 0, 3 + count: 1},
        compiler_params=LIMITS,
        name="over_rows",
    )(
        *[on_chip(v) for v in (gradient, *row_parts, columns, row_moment)],
        *([] if begin else [on_chip(new_rows)]), token,
    )


def over_columns(parts, col_moment, others, matrix, sizes, total_rows):
    mats, _, width, _ = sizes
    count = len(parts)

    def body(*refs):
        old = refs[count]
        new_cols, levels, lanes = refs[count + 1 + len(others) :][:3]
        both = added(part[...] for part in refs[:count])
        new = (
            second_decay * old[matrix : matrix + 1, :]
            + (1.0 - second_decay) * both[0:1, :width] / total_rows
        )
        new_cols[...] = new
        lanes[...] = lane_groups(both[1:2, :width] / new, width)
        level = jnp.sum(both[0:1, width:], axis=1, keepdims=True) / total_rows
        levels[...] = jnp.broadcast_to(level, (1, LANES))
        if others:
            for k, other in enumerate(refs[count + 1 :][: len(others)]):
                refs[-1][k : k + 1, :] = other[...]
            refs[-1][matrix : matrix + 1, :] = new

    outs = [chip_shape((1, width)), chip_shape((1, LANES)), chip_shape((1, LANES))]
    outs += [chip_shape((mats, width))] if others else []
    return pl.pallas_call(
        body,
        in_specs=[ON_CHIP] * (count + 1 + len(others)),
        out_specs=[ON_CHIP] * len(outs),
        out_shape=outs,
        compiler_params=LIMITS,
        name="over_columns",
    )(*[on_chip(v) for v in (*parts, col_moment, *others)])


def scale(scaled, new_cols, levels, clip_parts, output, matrix, sizes, total_rows):
    mats, rows, width, total_cols = sizes
    half_rows = rows // 2
    pieces = 4
    piece = half_rows // pieces
    count = len(clip_parts)
    begin = output is None

    def body(g, c, level, *refs):
        parts = refs[:count]
        out, ready, sent = refs[-3:]
        row_level = level[:, :1]
        clip = jnp.sum(added(p[...] for p in parts), axis=1, keepdims=True)
        clip = jnp.sqrt(clip * row_level / (total_rows * total_cols))
        factor = lax.rsqrt(c[...]) * (jnp.sqrt(row_level) / jnp.maximum(1.0, clip))

        def copy(half, k):
            at = pl.ds(half * half_rows + k * piece, piece)
            return pltpu.make_async_copy(
                ready.at[at], out.at[matrix, at], sent.at[half * pieces + k]
            )

        places = [(half, k) for half in range(2) for k in range(pieces)]
        for half, k in places:
            at = slice(k * piece, (k + 1) * piece)
            to = slice(half * half_rows + k * piece, half * half_rows + (k + 1) * piece)
            ready[to, :] = g[half, at, :] * factor
            copy(half, k).start()
        for place in places:
            copy(*place).wait()

    return pl.pallas_call(
        body,
        in_specs=[ON_CHIP] * (3 + count) + ([] if begin else [ANY]),
        out_specs=ANY,
        out_shape=hbm_shape((mats, rows, width)),
        input_output_aliases={} if begin else {3 + count: 0},
        scratch_shapes=[
            pltpu.VMEM((rows, width), jnp.float32),
            pltpu.SemaphoreType.DMA((2 * pieces,)),
        ],
        compiler_params=LIMITS,
        name="scale",
    )(
        *[on_chip(v) for v in (scaled, new_cols, levels, *clip_parts)],
        *([] if begin else [in_hbm(output)]),
    )


def chunks_of(mats):
    chunks = []
    for matrix in range(mats):
        start = 0
        for size in LAST if matrix == mats - 1 else FIRST:
            chunks.append((matrix, start, size))
            start += size
    return chunks


def kernel_order(count, bits):
    order = [("peer", 0), ("peer", 1)]
    for t in range(-2, count + max(bits, 1)):
        step = [(f"sum{k}", t - k + 1) for k in range(1, bits)]
        step += [("final", t - max(bits - 1, 0))]
        step += [("sum0", t + 2)] if bits else []
        step += [("peer", t + 3)]
        order += [
            (stage, i) for stage, i in step if 0 <= i < count and (stage, i) not in order
        ]
    return order


def rounds_after(n_col):
    return 5 * len(rounds_of(n_col)) - 2


def on_device(n_row, n_col, grad_terms, row_moment, col_moment):
    _, mats, rows, all_width = grad_terms.shape
    width = all_width // n_col
    half_rows = rows // 2
    bits = n_col.bit_length() - 2
    places = 1 << bits
    total_rows, total_cols = rows * n_row, all_width
    sizes = (mats, rows, width, total_cols)

    me = lax.axis_index("col").astype(jnp.int32)
    terms = grad_terms.reshape(mats, 2, half_rows, all_width)
    orders = (tuple(range(bits)), tuple(reversed(range(bits))))

    def place_mask(order, place):
        return sum(1 << bit for k, bit in enumerate(order) if place >> (bits - 1 - k) & 1)

    masks = [[2 * place_mask(order, p) for p in range(places)] for order in orders]
    table = jnp.bitwise_xor(jnp.array(masks, jnp.int32), me)

    unit = half_rows // 16
    chunks = [(m, start * unit, size * unit) for m, start, size in chunks_of(mats)]
    last_of = {c[0]: i for i, c in enumerate(chunks)}

    from_peer, received = {}, {i: [] for i in range(len(chunks))}
    totals, row_parts, scaled = [None] * mats, [None] * mats, [None] * mats
    moved, new_rows, new_cols = [], None, None
    token = in_hbm(terms)

    def divide_rows(matrix):
        nonlocal new_rows, new_cols, token
        gradient, _, columns = totals[matrix]
        scaled[matrix], new_rows, message = over_rows(
            gradient, row_parts[matrix], columns, row_moment, new_rows, token, matrix, sizes
        )
        token = on_chip(message)
        parts = sum_over(message, "row", n_row)
        others = [c for c, *_ in moved] if matrix == mats - 1 else []
        c, levels, lanes, *all_cols = over_columns(
            parts, col_moment, others, matrix, sizes, total_rows
        )
        new_cols = all_cols[0] if all_cols else c
        clip_parts = sum_over(lanes, "col", n_col)
        moved.append((c, levels, clip_parts))

    finished = []
    for stage, i in kernel_order(len(chunks), bits):
        for entry in finished:
            entry[1] -= 1
            if entry[1] == 0:
                divide_rows(entry[0])
        matrix = chunks[i][0]
        chip = i in ON_CHIP_CHUNKS or i - len(chunks) in ON_CHIP_CHUNKS
        put = on_chip if chip else in_hbm
        if stage == "peer":
            sent = peer_half(table, terms, token, chunks[i], places, width, chip)
        elif stage == "final":
            totals[matrix] = final_sums(
                table, terms, from_peer[i], received[i], totals[matrix], token,
                chunks[i], half_rows, width, chip,
            )
        else:
            k = int(stage[3:])
            sums = partial_sums(
                table, terms, from_peer[i], received[i], token, chunks[i],
                places >> (k + 1), width, chip,
            )
        if stage == "peer":
            token = put(sent)
            from_peer[i] = exchange(sent, "col", n_col, 1)
        elif stage == "final":
            token = on_chip(totals[matrix][2])
            if i == last_of[matrix]:
                row_parts[matrix] = sum_over(totals[matrix][1], "col", n_col)
                finished.append([matrix, rounds_after(n_col)])
        else:
            token = put(sums[0])
            received[i].append(
                [exchange(sums[half], "col", n_col, 2 << orders[half][k]) for half in range(2)]
            )
    for matrix in range(mats):
        if scaled[matrix] is None:
            divide_rows(matrix)

    update = None
    for matrix in range(mats):
        update = scale(
            scaled[matrix], *moved[matrix], update, matrix, sizes, total_rows
        )
    return update, new_rows, new_cols


def solution(mesh):
    n_row, n_col = mesh.shape["row"], mesh.shape["col"]
    placed = (P("col", None, "row", None), P(None, "row"), P(None, "col"))

    def body(*args):
        return on_device(n_row, n_col, *args)

    return jax.shard_map(
        body,
        mesh=mesh,
        in_specs=placed,
        out_specs=(P(None, "row", "col"), P(None, "row"), P(None, "col")),
        check_vma=False,
    )
```
